32 devices in a mesh: cp: 8 (over y, x, core), grp: 4 (over z).
Axes of the slice: x: 2, y: 2, z: 4, core: 2. Of those that a mesh axis runs over, the one named last changes fastest.
Arguments:
- queries: bfloat16 [4096, 2048], P(('cp', 'grp')), may hold values from -6 to 6
- keys: bfloat16 [4096, 512], P(('cp', 'grp')), may hold values from -6 to 6
- values: bfloat16 [4096, 512], P(('cp', 'grp')), may hold values from -6 to 6
- grad_out: bfloat16 [4096, 2048], P(('cp', 'grp')), may hold values from -6 to 6
- segments: int32 [4096], P(('cp', 'grp')), may hold values from 0 to 3, never falling along the last dimension, each value on 1 to 2048 neighbouring positions
- block_ids: int32 [32, 4], P(('cp', 'grp')), may hold values from 0 to 31, as said below
- block_count: int32 [32], P(('cp', 'grp')), may hold values from 1 to 4, as said below
Outputs:
- attended: bfloat16 [4096, 2048], P(('cp', 'grp'))
- grad_queries: bfloat16 [4096, 2048], P(('cp', 'grp'))
- grad_keys: bfloat16 [4096, 512], P(('cp', 'grp'))
- grad_values: bfloat16 [4096, 512], P(('cp', 'grp'))
The draws below stay inside these ranges and needn't reach their ends.
Inputs may be any that keep to these rules, and one draw needn't show every extreme that they name: `block_ids`: row t names tiles of its own neighbourhood (tiles 4 * (t // 4) onward, 4 of them) or of the neighbourhood before it; entry 0 is t itself; the first block_count[t] entries are distinct; later entries are ignored. `block_count`: reaches 4 in every draw.
All inputs are finite; a program needn't handle non-finite values.
Results may differ from the reference program's by a relative error of at most 0.012.
The reference program's roundings to bfloat16 on the way count: a program that leaves them out, or rounds other values in their place, can miss the bound.
Values may be sent and summed in bfloat16 or wider, within the bound.
No kernel may reach another device: no remote copies, remote signals or barrier semaphores. Data moves between devices by JAX's collectives and lax.ppermute only.
A program may use at most 64 MiB of HBM per device.

```python
import math
import jax
import jax.numpy as jnp
import numpy as np
from jax import lax

HEADS = 16
KV_HEADS = 4
HEAD = 128
BLOCK = 128
MAXB = 4
GROUP = 4
TILES = 32
TOKENS = 4096


def draw_queries(key, part):
    normal_part = jnp.clip(jax.random.normal(jax.random.fold_in(key, 1), (TOKENS, HEADS * HEAD), jnp.float32), -6.0, 6.0)
    return normal_part.astype(jnp.bfloat16)


def draw_keys(key, part):
    normal_part = jnp.clip(jax.random.normal(jax.random.fold_in(key, 2), (TOKENS, KV_HEADS * HEAD), jnp.float32), -6.0, 6.0)
    return normal_part.astype(jnp.bfloat16)


def draw_block_ids(key, part):
    tile_count = TILES
    own_tile = jnp.arange(tile_count, dtype=jnp.int32)
    candidate = jnp.arange(2 * GROUP, dtype=jnp.int32)
    named = (own_tile[:, None] // GROUP - 1) * GROUP + candidate[None, :]
    usable = (named >= 0) & (named != own_tile[:, None])
    noise = jax.random.randint(jax.random.fold_in(key, 5), (tile_count, 2 * GROUP), 0, 2 ** 20)
    scores = jnp.where(usable, noise * (2 * GROUP) + candidate[None, :], -1 - candidate[None, :])
    ranking = jnp.argsort(-scores, axis=1, stable=True)[:, :MAXB - 1]
    chosen = jnp.take_along_axis(named, ranking, axis=1)
    chosen_ok = jnp.take_along_axis(usable, ranking, axis=1)
    chosen = jnp.where(chosen_ok, chosen, own_tile[:, None])
    return jnp.concatenate([own_tile[:, None], chosen], axis=1).astype(jnp.int32)


def draw_block_count(key, part):
    tile_count = TILES
    own_tile = jnp.arange(tile_count, dtype=jnp.int32)
    heavy = jax.random.randint(jax.random.fold_in(key, 6), (tile_count,), 0, 4) == 0
    light = 1 + jax.random.randint(jax.random.fold_in(key, 7), (tile_count,), 0, 5)
    used = jnp.where(heavy, MAXB, jnp.minimum(light, MAXB))
    used = jnp.where(own_tile < GROUP, jnp.minimum(used, GROUP), used)
    used = used.at[tile_count - 1].set(MAXB)
    return used.astype(jnp.int32)


def block_levels(key, extent, cuts, low, high):
    def one(dim, shards_of):
        steps = jax.random.uniform(jax.random.fold_in(jax.random.fold_in(key, 6), dim), (shards_of,), jnp.float32, low / len(cuts), high / len(cuts))
        return jnp.repeat(jnp.exp(steps), extent[dim] // shards_of).reshape((-1,) + (1,) * (len(extent) - dim - 1))

    gain = one(*cuts[0])
    for cut in cuts[1:]:
        gain = gain * one(*cut)
    return gain


def profile(number_of, total, reach, lean):
    weights = [(1 << 20) // math.isqrt(standing ** lean) + 1 for standing in range(2, number_of + 1)]
    surplus, given = total - reach - (number_of - 1), [1] * (number_of - 1)
    while surplus > 0:
        movable = [i for i in range(number_of - 1) if given[i] < reach]
        mass, remaining = sum([weights[i] for i in movable]), surplus
        for i in movable:
            extra = min(reach - given[i], max(1, remaining * weights[i] // mass), surplus)
            given[i] = given[i] + extra
            surplus = surplus - extra
    return np.array([reach] + given)


def ragged_sizes(key, amount, total, reach, lean):
    if amount == 2:
        one = jax.random.randint(key, (), max(1, total - reach), min(reach, total - 1) + 1)
        return jnp.stack([one, total - one])
    tallies = jnp.asarray(profile(amount, total, reach, lean), jnp.int32)
    pairs = (amount - 1) // 2
    source_of, receiver = tallies[1:1 + 2 * pairs:2], tallies[2:2 + 2 * pairs:2]
    margin = jnp.minimum(source_of - 1, reach - receiver)
    shifted = jax.random.randint(jax.random.fold_in(key, 1), (pairs,), 0, 1 << 20) % (margin + 1)
    tallies = tallies.at[1:1 + 2 * pairs:2].set(source_of - shifted).at[2:2 + 2 * pairs:2].set(receiver + shifted)
    return tallies[jax.random.permutation(jax.random.fold_in(key, 2), amount)]


def centred(rng, extent, spread, reach, cuts=(), held_as=jnp.bfloat16):
    entries = jax.random.normal(rng, extent, jnp.float32) * spread
    if len(cuts) > 0:
        entries = block_levels(rng, extent, cuts, -0.22, 0.18) * entries
    return jnp.clip(entries, min=-reach, max=reach).astype(held_as)


def setup_inputs(seed: int = 0) -> dict:
    splits = jax.random.split(jax.random.key(seed), 8)
    return {
        "queries": draw_queries(jax.random.fold_in(splits[7], 71), 0),
        "keys": draw_keys(jax.random.fold_in(splits[7], 71), 0),
        "values": centred(splits[2], (TOKENS, KV_HEADS * HEAD), 1.0, 6.0, ((0, 32),)),
        "grad_out": centred(splits[3], (TOKENS, HEADS * HEAD), 1.0, 6.0, ((0, 32),)),
        "segments": jnp.searchsorted(jnp.cumsum(ragged_sizes(splits[4], max(TOKENS // (16 * BLOCK), 4), TOKENS, min(64 * BLOCK, TOKENS // 2), 2)), jnp.arange(TOKENS), side="right").astype(jnp.int32),
        "block_ids": draw_block_ids(jax.random.fold_in(splits[7], 71), 0),
        "block_count": draw_block_count(jax.random.fold_in(splits[7], 71), 0),
    }


NEG = -1.0e30


def attend_tile(query, grad_out, tile_keys, tile_values, query_seg, key_seg, is_live, kv_heads):
    tile_rows, full_width = query.shape
    slot_count, tile_size, kv_width = tile_keys.shape
    head_size = kv_width // kv_heads
    group_size = full_width // kv_width
    scaling = head_size ** -0.5
    key_slots = slot_count * tile_size
    allowed = (query_seg[:, None] == key_seg.reshape(key_slots)[None, :]) & jnp.repeat(is_live, tile_size)[None, :]
    query_heads = query.reshape(tile_rows, kv_heads, group_size, head_size).transpose(1, 0, 2, 3)
    grad_heads = grad_out.reshape(tile_rows, kv_heads, group_size, head_size).transpose(1, 0, 2, 3)
    key_heads = tile_keys.reshape(key_slots, kv_heads, head_size).transpose(1, 0, 2)
    value_heads = tile_values.reshape(key_slots, kv_heads, head_size).transpose(1, 0, 2)

    def per_head(pieces):
        query_one, grad_one, key_one, value_one = pieces
        query_f = query_one.astype(jnp.float32)
        grad_f = grad_one.astype(jnp.float32)
        key_f = key_one.astype(jnp.float32)
        value_f = value_one.astype(jnp.float32)
        scores = jnp.einsum("bge,ne->gbn", query_f, key_f) * scaling
        scores = jnp.where(allowed[None], scores, NEG)
        probability = jnp.exp(scores - jnp.max(scores, axis=-1, keepdims=True))
        probability = probability / jnp.sum(probability, axis=-1, keepdims=True)
        weights = lax.optimization_barrier(probability.astype(jnp.bfloat16)).astype(jnp.float32)
        attended = jnp.einsum("gbn,ne->bge", weights, value_f).astype(jnp.bfloat16)
        row_delta = jnp.sum(lax.optimization_barrier(attended).astype(jnp.float32) * grad_f, axis=-1)
        dprobs = jnp.einsum("bge,ne->gbn", grad_f, value_f)
        dscores = probability * (dprobs - row_delta.T[:, :, None])
        dscores = lax.optimization_barrier(dscores.astype(jnp.bfloat16)).astype(jnp.float32)
        grad_query = (jnp.einsum("gbn,ne->bge", dscores, key_f) * scaling).astype(jnp.bfloat16)
        key_term = jnp.einsum("gbn,bge->ne", dscores, query_f) * scaling
        value_term = jnp.einsum("gbn,bge->ne", weights, grad_f)
        return attended, grad_query, key_term, value_term

    attended, grad_query, key_term, value_term = lax.map(per_head, (query_heads, grad_heads, key_heads, value_heads))
    attended = attended.transpose(1, 0, 2, 3).reshape(tile_rows, full_width)
    grad_query = grad_query.transpose(1, 0, 2, 3).reshape(tile_rows, full_width)
    key_term = key_term.transpose(1, 0, 2).reshape(slot_count, tile_size, kv_width)
    value_term = value_term.transpose(1, 0, 2).reshape(slot_count, tile_size, kv_width)
    return attended, grad_query, key_term, value_term


def reference(queries, keys, values, grad_out, segments, block_ids, block_count):
    tile_count = TOKENS // BLOCK
    kv_width = keys.shape[1]
    key_tiles = keys.reshape(tile_count, BLOCK, kv_width)
    value_tiles = values.reshape(tile_count, BLOCK, kv_width)
    query_tiles = queries.reshape(tile_count, BLOCK, queries.shape[1])
    grad_tiles = grad_out.reshape(tile_count, BLOCK, queries.shape[1])
    seg_tiles = segments.reshape(tile_count, BLOCK)

    def advance(carry, pieces):
        key_sum, value_sum = carry
        query_t, grad_t, listed, used, seg_t = pieces
        is_live = jnp.arange(MAXB, dtype=jnp.int32) < used
        attended, grad_query, key_term, value_term = attend_tile(query_t, grad_t, key_tiles[listed], value_tiles[listed], seg_t, seg_tiles[listed], is_live, KV_HEADS)
        key_sum = key_sum.at[listed].add(lax.optimization_barrier(key_term.astype(jnp.bfloat16)).astype(jnp.float32))
        value_sum = value_sum.at[listed].add(lax.optimization_barrier(value_term.astype(jnp.bfloat16)).astype(jnp.float32))
        return (key_sum, value_sum), (attended, grad_query)

    start = jnp.zeros((tile_count, BLOCK, kv_width), jnp.float32)
    (key_sum, value_sum), (attended, grad_query) = lax.scan(advance, (start, start), (query_tiles, grad_tiles, block_ids, block_count, seg_tiles))
    attended = attended.reshape(TOKENS, queries.shape[1])
    grad_query = grad_query.reshape(TOKENS, queries.shape[1])
    grad_keys = key_sum.reshape(TOKENS, kv_width).astype(jnp.bfloat16)
    grad_values = value_sum.reshape(TOKENS, kv_width).astype(jnp.bfloat16)
    return attended, grad_query, grad_keys, grad_values
```

```python
import functools

import jax
import jax.numpy as jnp
from jax import lax
from jax.experimental import pallas as pl
from jax.experimental.pallas import tpu as pltpu
from jax.sharding import PartitionSpec as P


KV_HEADS = 4
CHUNKS = 1
SEG_ROWS = 8
NEG = -1e30
LOG2E = 1.4426950408889634

VMEM = pl.BlockSpec(memory_space=pltpu.VMEM)
SMEM = pl.BlockSpec(memory_space=pltpu.SMEM)
HBM = pl.BlockSpec(memory_space=pltpu.HBM)
F32 = jnp.float32
BF16 = jnp.bfloat16


def nbytes(*arrays):
    return sum(a.size * a.dtype.itemsize for a in arrays)


def call(kernel, outs, ins, in_specs, scratch=(), flops=0):
    cost = pl.CostEstimate(flops=flops, bytes_accessed=nbytes(*ins, *outs), transcendentals=0)
    return pl.pallas_call(
        kernel,
        out_shape=outs,
        in_specs=in_specs,
        out_specs=[VMEM] * len(outs),
        scratch_shapes=list(scratch),
        cost_estimate=cost,
        compiler_params=pltpu.CompilerParams(vmem_limit_bytes=32 * 1024 * 1024),
    )(*ins)


def pack_kernel(chunks, k_ref, v_ref, s_ref, *refs):
    outs, (seg, sems) = refs[:chunks], refs[chunks:]
    tile, kv = k_ref.shape
    part = kv // chunks
    copies = [pltpu.make_async_copy(s_ref, seg, sems.at[2 * chunks])]
    for i, out in enumerate(outs):
        cols = pl.ds(i * part, part)
        for j, ref in enumerate((k_ref, v_ref)):
            target = out.at[pl.ds(0, tile), pl.ds(j * part, part)]
            copies.append(pltpu.make_async_copy(ref.at[:, cols], target, sems.at[2 * i + j]))
    for copy in copies:
        copy.start()
    copies[0].wait()
    for out in outs:
        out[tile:, :] = jnp.zeros((SEG_ROWS, 2 * part), BF16)
        out[tile:, 0:tile] = jnp.broadcast_to(seg[...].astype(F32), (SEG_ROWS, tile)).astype(BF16)
    for copy in copies[1:]:
        copy.wait()


def attend_kernel(heads, group, ids_ref, count_ref, q_ref, g_ref, s_ref, *refs):
    tiles = 2 * group
    pool = refs[:tiles]
    att_ref, gq_ref = refs[tiles : tiles + 2]
    near = refs[tiles + 2 : tiles + 2 + group]
    far = refs[tiles + 2 + group : tiles + 2 + tiles]
    kv_s, seg_s, bias_s, term_s = refs[tiles + 2 + tiles :]
    tile = q_ref.shape[0]
    width = kv_s.shape[1]
    half = width // 2
    size = half // heads
    slots = ids_ref.shape[1]
    per = q_ref.shape[1] // half
    scaling = size ** (-0.5)

    me = lax.axis_index("grp")
    first = (lax.axis_index("cp") - 1) * group
    count = count_ref[0]

    def slot_of(place):
        steps, is_far = place % group, place >= group
        row = lax.rem(me - steps + group, group)
        want = first + row + (0 if is_far else group)
        found = jnp.int32(-1)
        for j in range(slots):
            found = jnp.where((ids_ref[0, j] == want) & (j < count), j, found)
        return found

    slot = [slot_of(p) for p in range(tiles)]
    for j in range(1, slots):

        @pl.when(j >= count)
        def _():
            kv_s[j * tile : (j + 1) * tile, :] = jnp.zeros((tile, width), BF16)
            seg_s[j] = jnp.full((SEG_ROWS, tile), -1.0, F32)

    for p in range(tiles):

        @pl.when(slot[p] >= 0)
        def _():
            start = pl.multiple_of(slot[p] * tile, tile)
            kv_s[pl.ds(start, tile), :] = pool[p][0:tile, :]
            seg_s[slot[p]] = pool[p][tile:, 0:tile].astype(F32)

    own = jnp.broadcast_to(s_ref[...].astype(F32), (tile, tile)).T
    for j in range(slots):
        bias_s[:, j * tile : (j + 1) * tile] = jnp.where(own == seg_s[j][0:1, :], 0.0, NEG)

    nt = (((1,), (1,)), ((), ()))
    for h in range(heads):
        k = kv_s[:, h * size : (h + 1) * size]
        v = kv_s[:, half + h * size : half + (h + 1) * size]
        span = range(h * per, (h + 1) * per)
        qs = jnp.concatenate([q_ref[:, x * size : (x + 1) * size] for x in span], axis=0)
        gs = jnp.concatenate([g_ref[:, x * size : (x + 1) * size] for x in span], axis=0)
        s = lax.dot_general(qs, k, nt, preferred_element_type=F32)
        dp = lax.dot_general(gs, v, nt, preferred_element_type=F32)
        bias = jnp.concatenate([bias_s[...]] * per, axis=0)
        s = s * (scaling * LOG2E) + bias
        e = jnp.exp2(s - jnp.max(s, axis=1, keepdims=True))
        p = e * (1.0 / jnp.sum(e, axis=1, keepdims=True))
        w = p.astype(BF16)
        a = jnp.dot(w, v, preferred_element_type=F32).astype(BF16)
        delta = jnp.sum(a.astype(F32) * gs.astype(F32), axis=1, keepdims=True)
        ds = (p * (dp - delta)).astype(BF16)
        gq = (jnp.dot(ds, k, preferred_element_type=F32) * scaling).astype(BF16)
        for i, x in enumerate(span):
            att_ref[:, x * size : (x + 1) * size] = a[i * tile : (i + 1) * tile]
            gq_ref[:, x * size : (x + 1) * size] = gq[i * tile : (i + 1) * tile]
        dk = jnp.dot(qs.T, ds, preferred_element_type=F32)
        term_s[:, h * size : (h + 1) * size] = (dk * scaling).T.astype(BF16)
        dv = jnp.dot(gs.T, w, preferred_element_type=F32)
        term_s[:, half + h * size : half + (h + 1) * size] = dv.T.astype(BF16)

    for p in range(tiles):
        out = near[p] if p < group else far[p - group]

        @pl.when(slot[p] >= 0)
        def _():
            out[...] = term_s[pl.ds(pl.multiple_of(slot[p] * tile, tile), tile), :]

        @pl.when(slot[p] < 0)
        def _():
            out[...] = jnp.zeros(out.shape, BF16)


def join_kernel(near, far, out):
    out[...] = (near[...].astype(F32) + far[...].astype(F32)).astype(out.dtype)


def total_kernel(chunks, parts, *refs):
    ins, (k_ref, v_ref) = refs[: chunks * parts], refs[chunks * parts :]
    part = k_ref.shape[1] // chunks
    for i in range(chunks):
        total = ins[i * parts][...]
        for one in ins[i * parts + 1 : (i + 1) * parts]:
            total += one[...].astype(F32)
        k_ref[:, i * part : (i + 1) * part] = total[:, :part].astype(BF16)
        v_ref[:, i * part : (i + 1) * part] = total[:, part:].astype(BF16)


def rotate(x, steps):
    count = lax.axis_size("grp")
    return lax.ppermute(x, "grp", [(i, (i + steps) % count) for i in range(count)])


def shift(x, steps):
    count = lax.axis_size("cp")
    return lax.ppermute(x, "cp", [(i, i + steps) for i in range(count) if 0 <= i + steps < count])


def near_first(group):
    order = []
    for d in range(1, group // 2 + 1):
        order += [d] if 2 * d == group else [d, group - d]
    return order


def body(queries, keys, values, grad_out, segments, block_ids, block_count):
    tile, kv = keys.shape
    full = queries.shape[1]
    group = lax.axis_size("grp")
    slots = block_ids.shape[1]
    heads = KV_HEADS // CHUNKS
    part = kv // CHUNKS
    width = 2 * part
    qpart = full // CHUNKS
    order = near_first(group)
    seg = segments.reshape(1, tile)
    payload = jax.ShapeDtypeStruct((tile + SEG_ROWS, width), BF16)
    packed = call(
        functools.partial(pack_kernel, CHUNKS),
        [payload] * CHUNKS,
        [keys, values, seg],
        [HBM] * 3,
        scratch=[pltpu.VMEM((1, tile), jnp.int32), pltpu.SemaphoreType.DMA((2 * CHUNKS + 1,))],
    )
    q_out = jax.ShapeDtypeStruct((tile, qpart), BF16)
    term = jax.ShapeDtypeStruct((tile, width), BF16)
    kept = jax.ShapeDtypeStruct((tile, width), F32)
    sums, att, gq = [], [], []
    for i in range(CHUNKS):
        near, far = [packed[i]] * group, [None] * group
        for d in order:
            near[d] = rotate(packed[i], d)
        for d in [0] + order:
            far[d] = shift(near[d], 1)
        cols = slice(i * qpart, (i + 1) * qpart)
        outs = call(
            functools.partial(attend_kernel, heads, group),
            [q_out, q_out] + [term] * (2 * group),
            [block_ids, block_count, queries[:, cols], grad_out[:, cols], seg, *near, *far],
            [SMEM, SMEM] + [VMEM] * (3 + 2 * group),
            scratch=[
                pltpu.VMEM((slots * tile, width), BF16),
                pltpu.VMEM((slots, SEG_ROWS, tile), F32),
                pltpu.VMEM((tile, slots * tile), F32),
                pltpu.VMEM((slots * tile, width), BF16),
            ],
            flops=12 * tile * slots * tile * qpart,
        )
        att.append(outs[0])
        gq.append(outs[1])
        near_terms, far_terms = outs[2 : 2 + group], outs[2 + group :]
        mine = [None] * group
        for d in order + [0]:
            later = shift(far_terms[d], -1)
            mine[d] = call(
                join_kernel, [term if d else kept], [near_terms[d], later], [VMEM] * 2
            )[0]
            if d:
                mine[d] = rotate(mine[d], -d)
        sums += mine
    dk, dv = call(
        functools.partial(total_kernel, CHUNKS, group),
        [jax.ShapeDtypeStruct((tile, kv), BF16)] * 2,
        sums,
        [VMEM] * len(sums),
    )
    if CHUNKS == 1:
        return att[0], gq[0], dk, dv
    return jnp.concatenate(att, axis=1), jnp.concatenate(gq, axis=1), dk, dv


def solution(mesh):
    two, one = P(("cp", "grp"), None), P(("cp", "grp"))
    return jax.shard_map(
        body,
        mesh=mesh,
        in_specs=(two, two, two, two, one, two, one),
        out_specs=(two,) * 4,
        check_vma=False,
    )
```

```python
import functools

import jax
import jax.numpy as jnp
from jax import lax
from jax.experimental import pallas as pl
from jax.experimental.pallas import tpu as pltpu
from jax.sharding import PartitionSpec as P


KV_HEADS = 4
PAIR = 2
BLOCK_ROWS = 64
NEG = -1e30
LOG2E = 1.4426950408889634

VMEM = pl.BlockSpec(memory_space=pltpu.VMEM)
SMEM = pl.BlockSpec(memory_space=pltpu.SMEM)
F32 = jnp.float32
BF16 = jnp.bfloat16


def call(kernel, outs, ins, in_specs=None, scratch=(), flops=0):
    bytes_accessed = sum(a.size * a.dtype.itemsize for a in [*ins, *outs])
    return pl.pallas_call(
        kernel,
        out_shape=outs,
        in_specs=in_specs or [VMEM] * len(ins),
        out_specs=[VMEM] * len(outs),
        scratch_shapes=list(scratch),
        cost_estimate=pl.CostEstimate(
            flops=flops, bytes_accessed=bytes_accessed, transcendentals=0
        ),
        compiler_params=pltpu.CompilerParams(vmem_limit_bytes=32 * 1024 * 1024),
    )(*ins)


def parity():
    return lax.rem(lax.axis_index("grp"), PAIR)


def part_of(index, width):
    return pl.ds(pl.multiple_of(index * width, width), width)


def pack_kernel(group, ids_ref, count_ref, k_ref, v_ref, s_ref, mine_ref, other_ref):
    tile, kv = k_ref.shape
    half = kv // PAIR
    slots = ids_ref.shape[1]
    first = (lax.axis_index("cp") - 1) * group
    notes = [s_ref[...].astype(F32)]
    for j in range(slots):
        notes.append(jnp.full((1, tile), ids_ref[0, j] - first, jnp.int32).astype(F32))
    notes.append(jnp.full((1, tile), count_ref[0], jnp.int32).astype(F32))
    extra = mine_ref.shape[0] - tile
    notes.append(jnp.zeros((extra - len(notes), tile), F32))
    notes = jnp.concatenate(notes, axis=0).astype(BF16)
    for index, out in ((parity(), mine_ref), (1 - parity(), other_ref)):
        out[0:tile, 0:half] = k_ref[:, part_of(index, half)]
        out[0:tile, half:] = v_ref[:, part_of(index, half)]
        out[tile:, :] = jnp.zeros((extra, 2 * half), BF16)
        out[tile:, 0:tile] = notes


def split_kernel(q_ref, g_ref, mine_ref, other_ref):
    tile, full = q_ref.shape
    half = full // PAIR
    size = mine_ref.shape[1]
    for index, out in ((parity(), mine_ref), (1 - parity(), other_ref)):
        for i, ref in enumerate((q_ref, g_ref)):
            for h in range(half // size):
                start = pl.multiple_of(index * half + h * size, size)
                top = (i * (half // size) + h) * tile
                out[top : top + tile, :] = ref[:, pl.ds(start, size)]


def merge_kernel(*refs):
    for i, ref in enumerate(refs[:-1]):
        refs[-1][i] = ref[...]


def attend_kernel(heads, group, partner, qg_ref, *refs):
    pool, far0, farm = refs[:group], refs[group], refs[group + 1]
    refs = refs[group + 2 :]
    if partner:
        before, refs = refs[: group + 1], refs[group + 1 :]
    ag_ref, near, far = refs[0], refs[1 : 1 + group], refs[1 + group]
    kv_s, seg_s, bias_s, term_s, p_s, dp_s, w_s, ds_s = refs[2 + group :]
    slots, width, tile = term_s.shape
    half = width // 2
    size = half // heads
    per = ag_ref.shape[1] // half
    rows = per * tile
    scaling = size ** (-0.5)
    me = lax.axis_index("grp")

    notes = pool[0][tile:, 0:tile]
    if partner:
        notes = jnp.where(parity() == 0, pool[group - 1][tile:, 0:tile], pool[1][tile:, 0:tile])
    notes = notes.astype(F32)
    listed = [jnp.max(notes[1 + j : 2 + j, :]).astype(jnp.int32) for j in range(slots)]
    count = jnp.max(notes[1 + slots : 2 + slots, :]).astype(jnp.int32)

    def slot_of(steps, offset):
        want = lax.rem(me - steps + group, group) + offset
        found = jnp.int32(-1)
        for j in range(slots):
            found = jnp.where((listed[j] == want) & (j < count), j, found)
        return found

    near_slot = [slot_of(d, group) for d in range(group)]
    far_slot = [slot_of(d, 0) for d in range(group)]
    for j in range(1, slots):

        @pl.when(j >= count)
        def _():
            kv_s[j * tile : (j + 1) * tile, :] = jnp.zeros((tile, width), BF16)
            seg_s[j] = jnp.full(seg_s.shape[1:], -1.0, F32)

    far_pool = [far0] + [farm.at[d] for d in range(group - 1)]
    for slot, source in zip(near_slot + far_slot, list(pool) + far_pool):

        @pl.when(slot >= 0)
        def _():
            kv_s[part_of(slot, tile), :] = source[0:tile, :]
            seg_s[slot] = source[tile:, 0:tile].astype(F32)

    own = jnp.broadcast_to(notes[0:1, :], (tile, tile)).T
    for j in range(slots):
        bias_s[:, j * tile : (j + 1) * tile] = jnp.where(own == seg_s[j][0:1, :], 0.0, NEG)

    nt = (((1,), (1,)), ((), ()))
    block = min(BLOCK_ROWS, tile)
    keys_of = lambda h: kv_s[:, h * size : (h + 1) * size]
    values_of = lambda h: kv_s[:, half + h * size : half + (h + 1) * size]
    queries_of = lambda h: qg_ref[h * rows : (h + 1) * rows, :]
    grads_of = lambda h: qg_ref[(heads + h) * rows : (heads + h + 1) * rows, :]

    def products(h):
        p_s[h] = lax.dot_general(queries_of(h), keys_of(h), nt, preferred_element_type=F32)
        dp_s[h] = lax.dot_general(grads_of(h), values_of(h), nt, preferred_element_type=F32)

    def weigh(h):
        for top in range(0, rows, block):
            over = slice(top, top + block)
            s = p_s[h, over, :] * (scaling * LOG2E) + bias_s[top % tile : top % tile + block, :]
            e = jnp.exp2(s - jnp.max(s, axis=1, keepdims=True))
            p = e * (1.0 / jnp.sum(e, axis=1, keepdims=True))
            p_s[h, over, :] = p
            w_s[h, over, :] = p.astype(BF16)

    def finish(h):
        a = jnp.dot(w_s[h], values_of(h), preferred_element_type=F32).astype(BF16)
        delta = jnp.sum(a.astype(F32) * grads_of(h).astype(F32), axis=1, keepdims=True)
        for top in range(0, rows, block):
            over = slice(top, top + block)
            ds = p_s[h, over, :] * (dp_s[h, over, :] - delta[over])
            ds_s[h, over, :] = ds.astype(BF16)
        dv = jnp.dot(grads_of(h).T, w_s[h], preferred_element_type=F32).astype(BF16)
        dk = jnp.dot(queries_of(h).T, ds_s[h], preferred_element_type=F32)
        dk = (dk * scaling).astype(BF16)
        for j in range(slots):
            keys = slice(j * tile, (j + 1) * tile)
            term_s[j, h * size : (h + 1) * size, :] = dk[:, keys]
            term_s[j, half + h * size : half + (h + 1) * size, :] = dv[:, keys]
        gq = (jnp.dot(ds_s[h], keys_of(h), preferred_element_type=F32) * scaling).astype(BF16)
        for i in range(per):
            x = h * per + i
            ag_ref[0:tile, x * size : (x + 1) * size] = a[i * tile : (i + 1) * tile]
            ag_ref[tile:, x * size : (x + 1) * size] = gq[i * tile : (i + 1) * tile]

    products(0)
    for h in range(heads):
        if h + 1 < heads:
            products(h + 1)
        weigh(h)
        finish(h)

    far_out = [far.at[d] for d in range(group)]
    if partner:
        old = list(before[:group]) + [before[group].at[d] for d in range(group)]
    for i, (slot, out) in enumerate(zip(near_slot + far_slot, list(near) + far_out)):

        @pl.when(slot >= 0)
        def _():
            new = term_s[slot].astype(F32)
            out[...] = (new + old[i][...] if partner else new).astype(out.dtype)

        @pl.when(slot < 0)
        def _():
            new = old[i][...] if partner else jnp.zeros((width, tile), F32)
            out[...] = new.astype(out.dtype)


def join_kernel(far, *refs):
    near, outs = refs[: len(refs) // 2], refs[len(refs) // 2 :]
    for d, (one, out) in enumerate(zip(near, outs)):
        out[...] = (one[...] + far[d].astype(F32)).astype(out.dtype)


def total_kernel(group, *refs):
    ins, (k_ref, v_ref) = refs[:group], refs[group:]
    tile, kv = k_ref.shape
    half = kv // PAIR
    for odd in range(PAIR):
        index = parity() if odd == 0 else 1 - parity()
        for top in range(0, half, tile):
            cols = pl.ds(pl.multiple_of(index * half + top, tile), tile)
            for ref, skip in ((k_ref, 0), (v_ref, half)):
                rows = slice(skip + top, skip + top + tile)
                total = ins[odd][rows, :].astype(F32)
                for one in ins[odd + PAIR :: PAIR]:
                    total += one[rows, :].astype(F32)
                ref[:, cols] = total.T.astype(BF16)


def unpack_kernel(mine_ref, other_ref, att_ref, gq_ref):
    tile, full = att_ref.shape
    half = full // PAIR
    for index, ref in ((parity(), mine_ref), (1 - parity(), other_ref)):
        att_ref[:, part_of(index, half)] = ref[0:tile, :]
        gq_ref[:, part_of(index, half)] = ref[tile:, :]


def body(queries, keys, values, grad_out, segments, block_ids, block_count):
    tile, kv = keys.shape
    full = queries.shape[1]
    group, cps = lax.axis_size("grp"), lax.axis_size("cp")
    slots = block_ids.shape[1]
    heads = KV_HEADS // PAIR
    size = kv // KV_HEADS
    width = 2 * kv // PAIR
    per = full // kv
    rows = per * tile
    shape = jax.ShapeDtypeStruct
    ahead = [(i, i + 1) for i in range(cps - 1)]
    back = [(b, a) for a, b in ahead]
    ring = lambda d: [(i, (i + d) % group) for i in range(group)]
    partners = [(i, i + 1 - 2 * (i % PAIR)) for i in range(group)]

    payload = shape((tile + -(-(slots + 2) // 8) * 8, width), BF16)
    mine, other = call(
        functools.partial(pack_kernel, group),
        [payload] * 2,
        [block_ids, block_count, keys, values, segments.reshape(1, tile)],
        in_specs=[SMEM] * 2 + [VMEM] * 3,
    )
    near = [mine]
    for d in range(1, group):
        near.append(lax.ppermute(other if d % PAIR else mine, "grp", ring(d)))
    qg = shape((2 * heads * rows, size), BF16)
    qg_mine, qg_other = call(split_kernel, [qg] * 2, [queries, grad_out])
    qg_partner = lax.ppermute(qg_other, "grp", partners)
    far0 = lax.ppermute(mine, "cp", ahead)
    merged = shape((group - 1, *payload.shape), BF16)
    (merged,) = call(merge_kernel, [merged], near[1:])
    farm = lax.ppermute(merged, "cp", ahead)

    ag = shape((2 * tile, full // PAIR), BF16)
    term = shape((width, tile), F32)
    scratch = [
        pltpu.VMEM((slots * tile, width), BF16),
        pltpu.VMEM((slots, payload.shape[0] - tile, tile), F32),
        pltpu.VMEM((tile, slots * tile), F32),
        pltpu.VMEM((slots, width, tile), BF16),
        pltpu.VMEM((heads, rows, slots * tile), F32),
        pltpu.VMEM((heads, rows, slots * tile), F32),
        pltpu.VMEM((heads, rows, slots * tile), BF16),
        pltpu.VMEM((heads, rows, slots * tile), BF16),
    ]
    flops = 12 * heads * rows * slots * tile * size
    ag_mine, *terms = call(
        functools.partial(attend_kernel, heads, group, False),
        [ag] + [term] * group + [shape((group, width, tile), F32)],
        [qg_mine, *near, far0, farm],
        scratch=scratch,
        flops=flops,
    )
    ag_partner, *terms = call(
        functools.partial(attend_kernel, heads, group, True),
        [ag] + [term] * group + [shape((group, width, tile), BF16)],
        [qg_partner, *near, far0, farm, *terms],
        scratch=scratch,
        flops=flops,
    )
    later = lax.ppermute(terms[group], "cp", back)
    ag_back = lax.ppermute(ag_partner, "grp", partners)
    joined = call(
        join_kernel, [term] + [shape((width, tile), BF16)] * (group - 1), [later, *terms[:group]]
    )
    sums = [joined[0]]
    for d in range(1, group):
        sums.append(lax.ppermute(joined[d], "grp", ring(-d)))
    out = shape((tile, full), BF16)
    attended, grad_queries = call(unpack_kernel, [out] * 2, [ag_mine, ag_back])
    grad = shape((tile, kv), BF16)
    dk, dv = call(functools.partial(total_kernel, group), [grad] * 2, sums)
    return attended, grad_queries, dk, dv


def solution(mesh):
    two, one = P(("cp", "grp"), None), P(("cp", "grp"))
    return jax.shard_map(
        body,
        mesh=mesh,
        in_specs=(two, two, two, two, one, two, one),
        out_specs=(two,) * 4,
        check_vma=False,
    )
```

```python
import functools

import jax
import jax.numpy as jnp
from jax import lax
from jax.experimental import pallas as pl
from jax.experimental.pallas import tpu as pltpu
from jax.sharding import PartitionSpec as P


KV_HEADS = 4
PAIR = 2
BLOCK_ROWS = 64
NEG = -1e30
LOG2E = 1.4426950408889634


VMEM = pl.BlockSpec(memory_space=pltpu.VMEM)
SMEM = pl.BlockSpec(memory_space=pltpu.SMEM)
F32 = jnp.float32
BF16 = jnp.bfloat16


def call(kernel, outs, ins, in_specs=None, scratch=(), flops=0):
    bytes_accessed = sum(a.size * a.dtype.itemsize for a in [*ins, *outs])
    return pl.pallas_call(
        kernel,
        out_shape=outs,
        in_specs=in_specs or [VMEM] * len(ins),
        out_specs=[VMEM] * len(outs),
        scratch_shapes=list(scratch),
        cost_estimate=pl.CostEstimate(
            flops=flops, bytes_accessed=bytes_accessed, transcendentals=0
        ),
        compiler_params=pltpu.CompilerParams(vmem_limit_bytes=32 * 1024 * 1024),
    )(*ins)


def parity():
    return lax.rem(lax.axis_index("grp"), PAIR)


def part_of(index, width):
    return pl.ds(pl.multiple_of(index * width, width), width)


def pack_kernel(group, ids_ref, count_ref, k_ref, v_ref, s_ref, mine_ref, other_ref):
    tile, kv = k_ref.shape
    half = kv // PAIR
    slots = ids_ref.shape[1]
    first = (lax.axis_index("cp") - 1) * group
    notes = [s_ref[...].astype(F32)]
    for j in range(slots):
        notes.append(jnp.full((1, tile), ids_ref[0, j] - first, jnp.int32).astype(F32))
    notes.append(jnp.full((1, tile), count_ref[0], jnp.int32).astype(F32))
    extra = mine_ref.shape[0] - tile
    notes.append(jnp.zeros((extra - len(notes), tile), F32))
    notes = jnp.concatenate(notes, axis=0).astype(BF16)
    for index, out in ((parity(), mine_ref), (1 - parity(), other_ref)):
        out[0:tile, 0:half] = k_ref[:, part_of(index, half)]
        out[0:tile, half:] = v_ref[:, part_of(index, half)]
        out[tile:, :] = jnp.zeros((extra, 2 * half), BF16)
        out[tile:, 0:tile] = notes


def split_kernel(q_ref, g_ref, mine_ref, other_ref):
    tile, full = q_ref.shape
    half = full // PAIR
    size = mine_ref.shape[1]
    for index, out in ((parity(), mine_ref), (1 - parity(), other_ref)):
        for i, ref in enumerate((q_ref, g_ref)):
            for h in range(half // size):
                start = pl.multiple_of(index * half + h * size, size)
                top = (i * (half // size) + h) * tile
                out[top : top + tile, :] = ref[:, pl.ds(start, size)]


def merge_kernel(*refs):
    for i, ref in enumerate(refs[:-1]):
        refs[-1][i] = ref[...]


def merge(arrays):
    out = jax.ShapeDtypeStruct((len(arrays), *arrays[0].shape), arrays[0].dtype)
    return call(merge_kernel, [out], arrays)[0]


def entries(refs, groups):
    places = {d: ref.at[i] for ref, group in zip(refs, groups) for i, d in enumerate(group)}
    return [places[d] for d in sorted(places)]


def attend_kernel(heads, group, far_in, far_out, partner, qg_ref, *refs):
    pool, refs = refs[:group], refs[group:]
    far_pool, refs = entries(refs[: len(far_in)], far_in), refs[len(far_in) :]
    parts = group + len(far_out)
    if partner:
        old, refs = refs[:parts], refs[parts:]
        old = [*old[:group], *entries(old[group:], far_out)]
    ag_ref, out, refs = refs[0], refs[1 : 1 + parts], refs[1 + parts :]
    out = [*out[:group], *entries(out[group:], far_out)]
    kv_s, seg_s, bias_s, term_s, p_s, dp_s, w_s, ds_s = refs
    slots, width, tile = term_s.shape
    half = width // 2
    size = half // heads
    per = ag_ref.shape[1] // half
    rows = per * tile
    scaling = size ** (-0.5)
    me = lax.axis_index("grp")

    notes = pool[0][tile:, 0:tile]
    if partner:
        notes = jnp.where(parity() == 0, pool[group - 1][tile:, 0:tile], pool[1][tile:, 0:tile])
    notes = notes.astype(F32)
    listed = [jnp.max(notes[1 + j : 2 + j, :]).astype(jnp.int32) for j in range(slots)]
    count = jnp.max(notes[1 + slots : 2 + slots, :]).astype(jnp.int32)

    def slot_of(steps, offset):
        want = lax.rem(me - steps + group, group) + offset
        found = jnp.int32(-1)
        for j in range(slots):
            found = jnp.where((listed[j] == want) & (j < count), j, found)
        return found

    near_slot = [slot_of(d, group) for d in range(group)]
    far_slot = [slot_of(d, 0) for d in range(group)]
    for j in range(1, slots):

        @pl.when(j >= count)
        def _():
            kv_s[j * tile : (j + 1) * tile, :] = jnp.zeros((tile, width), BF16)
            seg_s[j] = jnp.full(seg_s.shape[1:], -1.0, F32)

    for slot, source in zip(near_slot + far_slot, [*pool, *far_pool]):

        @pl.when(slot >= 0)
        def _():
            kv_s[part_of(slot, tile), :] = source[0:tile, :]
            seg_s[slot] = source[tile:, 0:tile].astype(F32)

    own = jnp.broadcast_to(notes[0:1, :], (tile, tile)).T
    for j in range(slots):
        bias_s[:, j * tile : (j + 1) * tile] = jnp.where(own == seg_s[j][0:1, :], 0.0, NEG)

    nt = (((1,), (1,)), ((), ()))
    block = min(BLOCK_ROWS, tile)
    keys_of = lambda h: kv_s[:, h * size : (h + 1) * size]
    values_of = lambda h: kv_s[:, half + h * size : half + (h + 1) * size]
    queries_of = lambda h: qg_ref[h * rows : (h + 1) * rows, :]
    grads_of = lambda h: qg_ref[(heads + h) * rows : (heads + h + 1) * rows, :]

    def products(h):
        p_s[h] = lax.dot_general(queries_of(h), keys_of(h), nt, preferred_element_type=F32)
        dp_s[h] = lax.dot_general(grads_of(h), values_of(h), nt, preferred_element_type=F32)

    def weigh(h):
        for top in range(0, rows, block):
            over = slice(top, top + block)
            s = p_s[h, over, :] * (scaling * LOG2E) + bias_s[top % tile : top % tile + block, :]
            e = jnp.exp2(s - jnp.max(s, axis=1, keepdims=True))
            p = e * (1.0 / jnp.sum(e, axis=1, keepdims=True))
            p_s[h, over, :] = p
            w_s[h, over, :] = p.astype(BF16)

    def finish(h):
        a = jnp.dot(w_s[h], values_of(h), preferred_element_type=F32).astype(BF16)
        delta = jnp.sum(a.astype(F32) * grads_of(h).astype(F32), axis=1, keepdims=True)
        for top in range(0, rows, block):
            over = slice(top, top + block)
            ds = p_s[h, over, :] * (dp_s[h, over, :] - delta[over])
            ds_s[h, over, :] = ds.astype(BF16)
        dv = jnp.dot(grads_of(h).T, w_s[h], preferred_element_type=F32).astype(BF16)
        dk = jnp.dot(queries_of(h).T, ds_s[h], preferred_element_type=F32)
        dk = (dk * scaling).astype(BF16)
        for j in range(slots):
            keys = slice(j * tile, (j + 1) * tile)
            term_s[j, h * size : (h + 1) * size, :] = dk[:, keys]
            term_s[j, half + h * size : half + (h + 1) * size, :] = dv[:, keys]
        gq = (jnp.dot(ds_s[h], keys_of(h), preferred_element_type=F32) * scaling).astype(BF16)
        for i in range(per):
            x = h * per + i
            ag_ref[0:tile, x * size : (x + 1) * size] = a[i * tile : (i + 1) * tile]
            ag_ref[tile:, x * size : (x + 1) * size] = gq[i * tile : (i + 1) * tile]

    products(0)
    for h in range(heads):
        if h + 1 < heads:
            products(h + 1)
        weigh(h)
        finish(h)

    for i, slot in enumerate(near_slot + far_slot):

        @pl.when(slot >= 0)
        def _():
            new = term_s[slot].astype(F32)
            out[i][...] = (new + old[i][...] if partner else new).astype(out[i].dtype)

        @pl.when(slot < 0)
        def _():
            new = old[i][...] if partner else jnp.zeros((width, tile), F32)
            out[i][...] = new.astype(out[i].dtype)


def join_kernel(far, *refs):
    near, outs = refs[: len(refs) // 2], refs[len(refs) // 2 :]
    for d, (one, out) in enumerate(zip(near, outs)):
        out[...] = (one[...] + far[d].astype(F32)).astype(out.dtype)


def total_kernel(group, *refs):
    ins, (k_ref, v_ref) = refs[:group], refs[group:]
    tile, kv = k_ref.shape
    half = kv // PAIR
    for odd in range(PAIR):
        index = parity() if odd == 0 else 1 - parity()
        for top in range(0, half, tile):
            cols = pl.ds(pl.multiple_of(index * half + top, tile), tile)
            for ref, skip in ((k_ref, 0), (v_ref, half)):
                rows = slice(skip + top, skip + top + tile)
                total = ins[odd][rows, :].astype(F32)
                for one in ins[odd + PAIR :: PAIR]:
                    total += one[rows, :].astype(F32)
                ref[:, cols] = total.T.astype(BF16)


def unpack_kernel(mine_ref, other_ref, att_ref, gq_ref):
    tile, full = att_ref.shape
    half = full // PAIR
    for index, ref in ((parity(), mine_ref), (1 - parity(), other_ref)):
        att_ref[:, part_of(index, half)] = ref[0:tile, :]
        gq_ref[:, part_of(index, half)] = ref[tile:, :]


def turns_of(group):
    turns = sorted(range(1, group), key=lambda d: (min(d, group - d), d))
    return turns[:2], turns[2:]


def body(queries, keys, values, grad_out, segments, block_ids, block_count):
    tile, kv = keys.shape
    full = queries.shape[1]
    group, cps = lax.axis_size("grp"), lax.axis_size("cp")
    slots = block_ids.shape[1]
    heads = KV_HEADS // PAIR
    size = kv // KV_HEADS
    width = 2 * kv // PAIR
    per = full // kv
    rows = per * tile
    shape = jax.ShapeDtypeStruct
    ahead = [(i, i + 1) for i in range(cps - 1)]
    back = [(b, a) for a, b in ahead]
    ring = lambda d: [(i, (i + d) % group) for i in range(group)]
    partners = [(i, i + 1 - 2 * (i % PAIR)) for i in range(group)]

    queries, keys, values, grad_out, segments, block_ids = (
        pltpu.with_memory_space_constraint(x, pltpu.HBM)
        for x in (queries, keys, values, grad_out, segments.reshape(1, tile), block_ids)
    )
    payload = shape((tile + -(-(slots + 2) // 8) * 8, width), BF16)
    mine, other = call(
        functools.partial(pack_kernel, group),
        [payload] * 2,
        [block_ids, block_count, keys, values, segments],
        in_specs=[SMEM] * 2 + [VMEM] * 3,
    )
    first, rest = turns_of(group)
    near = [mine]
    for d in range(1, group):
        near.append(lax.ppermute(other if d % PAIR else mine, "grp", ring(d)))
    qg = shape((2 * heads * rows, size), BF16)
    qg_mine, qg_other = call(split_kernel, [qg] * 2, [queries, grad_out])
    qg_partner = lax.ppermute(qg_other, "grp", partners)
    far_in = [g for g in ([0], first, rest) if g]
    far = [lax.ppermute(merge([near[d] for d in g]), "cp", ahead) for g in far_in]
    far_out = [g for g in (first, [0] + rest) if g]

    ag = shape((2 * tile, full // PAIR), BF16)
    term = shape((width, tile), F32)
    scratch = [
        pltpu.VMEM((slots * tile, width), BF16),
        pltpu.VMEM((slots, payload.shape[0] - tile, tile), F32),
        pltpu.VMEM((tile, slots * tile), F32),
        pltpu.VMEM((slots, width, tile), BF16),
        pltpu.VMEM((heads, rows, slots * tile), F32),
        pltpu.VMEM((heads, rows, slots * tile), F32),
        pltpu.VMEM((heads, rows, slots * tile), BF16),
        pltpu.VMEM((heads, rows, slots * tile), BF16),
    ]
    flops = 12 * heads * rows * slots * tile * size

    def attend(qg, before, dtype):
        return call(
            functools.partial(attend_kernel, heads, group, far_in, far_out, bool(before)),
            [ag] + [term] * group + [shape((len(g), width, tile), dtype) for g in far_out],
            [qg, *near, *far, *before],
            scratch=scratch,
            flops=flops,
        )

    ag_mine, *terms = attend(qg_mine, [], F32)
    ag_partner, *terms = attend(qg_partner, terms, BF16)
    ag_back = lax.ppermute(ag_partner, "grp", partners)
    joined = {}
    for g, far_terms in zip(far_out, terms[group:]):
        later = lax.ppermute(far_terms, "cp", back)
        outs = [term if d == 0 else shape((width, tile), BF16) for d in g]
        joined.update(zip(g, call(join_kernel, outs, [later] + [terms[d] for d in g])))
    sums = [joined[0]]
    for d in range(1, group):
        sums.append(lax.ppermute(joined[d], "grp", ring(-d)))
    out = shape((tile, full), BF16)
    attended, grad_queries = call(unpack_kernel, [out] * 2, [ag_mine, ag_back])
    grad = shape((tile, kv), BF16)
    dk, dv = call(functools.partial(total_kernel, group), [grad] * 2, sums)
    return attended, grad_queries, dk, dv


def solution(mesh):
    two, one = P(("cp", "grp"), None), P(("cp", "grp"))
    return jax.shard_map(
        body,
        mesh=mesh,
        in_specs=(two, two, two, two, one, two, one),
        out_specs=(two,) * 4,
        check_vma=False,
    )
```

```python
import functools

import jax
import jax.numpy as jnp
from jax import lax
from jax.experimental import pallas as pl
from jax.experimental.pallas import tpu as pltpu
from jax.sharding import PartitionSpec as P


KV_HEADS = 4
PAIR = 2
BLOCK_ROWS = 64
NEG = -1e30
LOG2E = 1.4426950408889634


VMEM = pl.BlockSpec(memory_space=pltpu.VMEM)
SMEM = pl.BlockSpec(memory_space=pltpu.SMEM)
F32 = jnp.float32
BF16 = jnp.bfloat16


def call(kernel, outs, ins, in_specs=None, scratch=(), flops=0):
    bytes_accessed = sum(a.size * a.dtype.itemsize for a in [*ins, *outs])
    return pl.pallas_call(
        kernel,
        out_shape=outs,
        in_specs=in_specs or [VMEM] * len(ins),
        out_specs=[VMEM] * len(outs),
        scratch_shapes=list(scratch),
        cost_estimate=pl.CostEstimate(
            flops=flops, bytes_accessed=bytes_accessed, transcendentals=0
        ),
        compiler_params=pltpu.CompilerParams(vmem_limit_bytes=32 * 1024 * 1024),
    )(*ins)


def parity():
    return lax.rem(lax.axis_index("grp"), PAIR)


def part_of(index, width):
    return pl.ds(pl.multiple_of(index * width, width), width)


def pack_kernel(group, ids_ref, count_ref, k_ref, v_ref, s_ref, mine_ref, other_ref):
    tile, kv = k_ref.shape
    half = kv // PAIR
    slots = ids_ref.shape[1]
    first = (lax.axis_index("cp") - 1) * group
    notes = [s_ref[...].astype(F32)]
    for j in range(slots):
        notes.append(jnp.full((1, tile), ids_ref[0, j] - first, jnp.int32).astype(F32))
    notes.append(jnp.full((1, tile), count_ref[0], jnp.int32).astype(F32))
    extra = mine_ref.shape[0] - tile
    notes.append(jnp.zeros((extra - len(notes), tile), F32))
    notes = jnp.concatenate(notes, axis=0).astype(BF16)
    for index, out in ((parity(), mine_ref), (1 - parity(), other_ref)):
        out[0:tile, 0:half] = k_ref[:, part_of(index, half)]
        out[0:tile, half:] = v_ref[:, part_of(index, half)]
        out[tile:, :] = jnp.zeros((extra, 2 * half), BF16)
        out[tile:, 0:tile] = notes


def split_kernel(q_ref, g_ref, mine_ref, other_ref):
    tile, full = q_ref.shape
    half = full // PAIR
    size = mine_ref.shape[1]
    for index, out in ((parity(), mine_ref), (1 - parity(), other_ref)):
        for i, ref in enumerate((q_ref, g_ref)):
            for h in range(half // size):
                start = pl.multiple_of(index * half + h * size, size)
                top = (i * (half // size) + h) * tile
                out[top : top + tile, :] = ref[:, pl.ds(start, size)]


def merge_kernel(*refs):
    for i, ref in enumerate(refs[:-1]):
        refs[-1][i] = ref[...]


def merge(arrays):
    out = jax.ShapeDtypeStruct((len(arrays), *arrays[0].shape), arrays[0].dtype)
    return call(merge_kernel, [out], arrays)[0]


def entries(refs, groups):
    places = {d: ref.at[i] for ref, group in zip(refs, groups) for i, d in enumerate(group)}
    return [places[d] for d in sorted(places)]


def attend_kernel(heads, group, far_in, far_out, partner, qg_ref, *refs):
    pool, refs = refs[:group], refs[group:]
    far_pool, refs = entries(refs[: len(far_in)], far_in), refs[len(far_in) :]
    parts = group + len(far_out)
    if partner:
        own_terms, refs = refs[0], refs[1:]
        ag_ref, out, refs = refs[0], refs[1 : 1 + parts], refs[1 + parts :]
        out = [*out[:group], *entries(out[group:], far_out)]
        term_s, refs = refs[0], refs[1:]
    else:
        ag_ref, term_s, refs = refs[0], refs[1], refs[2:]
    kv_s, seg_s, bias_s, p_s, dp_s, w_s, ds_s = refs
    slots, width, tile = term_s.shape
    half = width // 2
    size = half // heads
    per = ag_ref.shape[1] // half
    rows = per * tile
    scaling = size ** (-0.5)
    me = lax.axis_index("grp")

    def read(notes):
        listed = [jnp.max(notes[1 + j : 2 + j, :]).astype(jnp.int32) for j in range(slots)]
        count = jnp.max(notes[1 + slots : 2 + slots, :]).astype(jnp.int32)
        found = []
        for offset in (group, 0):
            for d in range(group):
                want = lax.rem(me - d + group, group) + offset
                slot = jnp.int32(-1)
                for j in range(slots):
                    slot = jnp.where((listed[j] == want) & (j < count), j, slot)
                found.append(slot)
        return count, found

    mine = pool[0][tile:, 0:tile].astype(F32)
    notes = mine
    if partner:
        notes = jnp.where(parity() == 0, pool[group - 1][tile:, 0:tile], pool[1][tile:, 0:tile])
        notes = notes.astype(F32)
    count, found = read(notes)
    for j in range(1, slots):

        @pl.when(j >= count)
        def _():
            kv_s[j * tile : (j + 1) * tile, :] = jnp.zeros((tile, width), BF16)
            seg_s[j] = jnp.full(seg_s.shape[1:], -1.0, F32)

    for slot, source in zip(found, [*pool, *far_pool]):

        @pl.when(slot >= 0)
        def _():
            kv_s[part_of(slot, tile), :] = source[0:tile, :]
            seg_s[slot] = source[tile:, 0:tile].astype(F32)

    own = jnp.broadcast_to(notes[0:1, :], (tile, tile)).T
    for j in range(slots):
        bias_s[:, j * tile : (j + 1) * tile] = jnp.where(own == seg_s[j][0:1, :], 0.0, NEG)

    nt = (((1,), (1,)), ((), ()))
    block = min(BLOCK_ROWS, tile)
    keys_of = lambda h: kv_s[:, h * size : (h + 1) * size]
    values_of = lambda h: kv_s[:, half + h * size : half + (h + 1) * size]
    queries_of = lambda h: qg_ref[h * rows : (h + 1) * rows, :]
    grads_of = lambda h: qg_ref[(heads + h) * rows : (heads + h + 1) * rows, :]

    def products(h):
        p_s[h] = lax.dot_general(queries_of(h), keys_of(h), nt, preferred_element_type=F32)
        dp_s[h] = lax.dot_general(grads_of(h), values_of(h), nt, preferred_element_type=F32)

    def weigh(h):
        for top in range(0, rows, block):
            over = slice(top, top + block)
            s = p_s[h, over, :] * (scaling * LOG2E) + bias_s[top % tile : top % tile + block, :]
            e = jnp.exp2(s - jnp.max(s, axis=1, keepdims=True))
            p = e * (1.0 / jnp.sum(e, axis=1, keepdims=True))
            p_s[h, over, :] = p
            w_s[h, over, :] = p.astype(BF16)

    def finish(h):
        a = jnp.dot(w_s[h], values_of(h), preferred_element_type=F32).astype(BF16)
        delta = jnp.sum(a.astype(F32) * grads_of(h).astype(F32), axis=1, keepdims=True)
        for top in range(0, rows, block):
            over = slice(top, top + block)
            ds = p_s[h, over, :] * (dp_s[h, over, :] - delta[over])
            ds_s[h, over, :] = ds.astype(BF16)
        dv = jnp.dot(grads_of(h).T, w_s[h], preferred_element_type=F32).astype(BF16)
        dk = jnp.dot(queries_of(h).T, ds_s[h], preferred_element_type=F32)
        dk = (dk * scaling).astype(BF16)
        for j in range(slots):
            keys = slice(j * tile, (j + 1) * tile)
            term_s[j, h * size : (h + 1) * size, :] = dk[:, keys]
            term_s[j, half + h * size : half + (h + 1) * size, :] = dv[:, keys]
        gq = (jnp.dot(ds_s[h], keys_of(h), preferred_element_type=F32) * scaling).astype(BF16)
        for i in range(per):
            x = h * per + i
            ag_ref[0:tile, x * size : (x + 1) * size] = a[i * tile : (i + 1) * tile]
            ag_ref[tile:, x * size : (x + 1) * size] = gq[i * tile : (i + 1) * tile]

    products(0)
    for h in range(heads):
        if h + 1 < heads:
            products(h + 1)
        weigh(h)
        finish(h)

    if not partner:
        return
    for slot, own_slot, target in zip(found, read(mine)[1], out):
        here, there = term_s.at[jnp.maximum(slot, 0)], own_terms.at[jnp.maximum(own_slot, 0)]

        @pl.when((slot >= 0) & (own_slot >= 0))
        def _():
            target[...] = (here[...].astype(F32) + there[...].astype(F32)).astype(target.dtype)

        @pl.when((slot >= 0) & (own_slot < 0))
        def _():
            target[...] = here[...].astype(target.dtype)

        @pl.when((slot < 0) & (own_slot >= 0))
        def _():
            target[...] = there[...].astype(target.dtype)

        @pl.when((slot < 0) & (own_slot < 0))
        def _():
            target[...] = jnp.zeros((width, tile), target.dtype)


def join_kernel(far, *refs):
    near, outs = refs[: len(refs) // 2], refs[len(refs) // 2 :]
    for d, (one, out) in enumerate(zip(near, outs)):
        out[...] = (one[...] + far[d].astype(F32)).astype(out.dtype)


def total_kernel(group, *refs):
    ins, (k_ref, v_ref) = refs[:group], refs[group:]
    tile, kv = k_ref.shape
    half = kv // PAIR
    for odd in range(PAIR):
        index = parity() if odd == 0 else 1 - parity()
        for top in range(0, half, tile):
            cols = pl.ds(pl.multiple_of(index * half + top, tile), tile)
            for ref, skip in ((k_ref, 0), (v_ref, half)):
                rows = slice(skip + top, skip + top + tile)
                total = ins[odd][rows, :].astype(F32)
                for one in ins[odd + PAIR :: PAIR]:
                    total += one[rows, :].astype(F32)
                ref[:, cols] = total.T.astype(BF16)


def unpack_kernel(mine_ref, other_ref, att_ref, gq_ref):
    tile, full = att_ref.shape
    half = full // PAIR
    for index, ref in ((parity(), mine_ref), (1 - parity(), other_ref)):
        att_ref[:, part_of(index, half)] = ref[0:tile, :]
        gq_ref[:, part_of(index, half)] = ref[tile:, :]


def turns_of(group):
    turns = sorted(range(1, group), key=lambda d: (min(d, group - d), d))
    return turns[:2], turns[2:]


def body(queries, keys, values, grad_out, segments, block_ids, block_count):
    tile, kv = keys.shape
    full = queries.shape[1]
    group, cps = lax.axis_size("grp"), lax.axis_size("cp")
    slots = block_ids.shape[1]
    heads = KV_HEADS // PAIR
    size = kv // KV_HEADS
    width = 2 * kv // PAIR
    per = full // kv
    rows = per * tile
    shape = jax.ShapeDtypeStruct
    ahead = [(i, i + 1) for i in range(cps - 1)]
    back = [(b, a) for a, b in ahead]
    ring = lambda d: [(i, (i + d) % group) for i in range(group)]
    partners = [(i, i + 1 - 2 * (i % PAIR)) for i in range(group)]

    queries, keys, values, grad_out, segments, block_ids = (
        pltpu.with_memory_space_constraint(x, pltpu.HBM)
        for x in (queries, keys, values, grad_out, segments.reshape(1, tile), block_ids)
    )
    payload = shape((tile + -(-(slots + 2) // 8) * 8, width), BF16)
    mine, other = call(
        functools.partial(pack_kernel, group),
        [payload] * 2,
        [block_ids, block_count, keys, values, segments],
        in_specs=[SMEM] * 2 + [VMEM] * 3,
    )
    first, rest = turns_of(group)
    near = [mine]
    for d in range(1, group):
        near.append(lax.ppermute(other if d % PAIR else mine, "grp", ring(d)))
    qg = shape((2 * heads * rows, size), BF16)
    qg_mine, qg_other = call(split_kernel, [qg] * 2, [queries, grad_out])
    qg_partner = lax.ppermute(qg_other, "grp", partners)
    far_in = [g for g in ([0], first, rest) if g]
    far = [lax.ppermute(merge([near[d] for d in g]), "cp", ahead) for g in far_in]
    far_out = [g for g in (rest + first[1:], first[:1] + [0]) if g]

    ag = shape((2 * tile, full // PAIR), BF16)
    term = shape((width, tile), F32)
    scratch = [
        pltpu.VMEM((slots * tile, width), BF16),
        pltpu.VMEM((slots, payload.shape[0] - tile, tile), F32),
        pltpu.VMEM((tile, slots * tile), F32),
        pltpu.VMEM((heads, rows, slots * tile), F32),
        pltpu.VMEM((heads, rows, slots * tile), F32),
        pltpu.VMEM((heads, rows, slots * tile), BF16),
        pltpu.VMEM((heads, rows, slots * tile), BF16),
    ]
    flops = 12 * heads * rows * slots * tile * size

    def attend(partner, qg, outs, extra, extra_scratch):
        return call(
            functools.partial(attend_kernel, heads, group, far_in, far_out, partner),
            [ag, *outs],
            [qg, *near, *far, *extra],
            scratch=extra_scratch + scratch,
            flops=flops,
        )

    listed = (slots, width, tile)
    ag_mine, own_terms = attend(False, qg_mine, [shape(listed, BF16)], [], [])
    outs = [term] * group + [shape((len(g), width, tile), BF16) for g in far_out]
    ag_partner, *terms = attend(True, qg_partner, outs, [own_terms], [pltpu.VMEM(listed, BF16)])
    ag_back = lax.ppermute(ag_partner, "grp", partners)
    joined = {}
    for g, far_terms in zip(far_out, terms[group:]):
        later = lax.ppermute(far_terms, "cp", back)
        outs = [term if d == 0 else shape((width, tile), BF16) for d in g]
        joined.update(zip(g, call(join_kernel, outs, [later] + [terms[d] for d in g])))
    sums = [joined[0]]
    for d in range(1, group):
        sums.append(lax.ppermute(joined[d], "grp", ring(-d)))
    out = shape((tile, full), BF16)
    attended, grad_queries = call(unpack_kernel, [out] * 2, [ag_mine, ag_back])
    grad = shape((tile, kv), BF16)
    dk, dv = call(functools.partial(total_kernel, group), [grad] * 2, sums)
    return attended, grad_queries, dk, dv


def solution(mesh):
    two, one = P(("cp", "grp"), None), P(("cp", "grp"))
    return jax.shard_map(
        body,
        mesh=mesh,
        in_specs=(two, two, two, two, one, two, one),
        out_specs=(two,) * 4,
        check_vma=False,
    )
```
